8 devices in a mesh: data: 1 (over z), tp: 2 (over y), cp: 4 (over x, core).
Axes of the slice: x: 2, y: 2, z: 1, core: 2. Of those that a mesh axis runs over, the one named last changes fastest.
Arguments:
- x: bfloat16 [16, 1024, 5120], P('data', ('cp', 'tp'))
- positions: int32 [16, 1024], P('data', ('cp', 'tp'))
- w_query: bfloat16 [5120, 5120], P(None, 'tp')
- w_key: bfloat16 [5120, 1024], P(None, 'tp')
- w_value: bfloat16 [5120, 1024], P(None, 'tp')
- w_out: bfloat16 [5120, 5120], P('tp')
Outputs:
- output: bfloat16 [16, 1024, 5120], P('data', ('cp', 'tp'))
All inputs are finite; a program needn't handle non-finite values.
Results may differ from the reference program's by a relative error of at most 0.00658.
Values are sent between devices in bfloat16 or wider.
A program may use at most 1 GiB of HBM per device.

```python
import math
import jax
import jax.numpy as jnp
from jax import lax

BATCH_ROWS = 16
CHUNK_LEN = 128
CP_SIZE = 4
MODEL_DIM = 5120
Q_HEADS = 40
KV_HEADS = 8
HEAD_DIM = 128
ROPE_BASE = 500000
WALK_RANK = 64
SEQ_LEN = 2 * CP_SIZE * CHUNK_LEN
Q_PER_KV = Q_HEADS // KV_HEADS
N_BLOCKS = SEQ_LEN // CHUNK_LEN


def to_storage_order(seq_vals):
    trailing = seq_vals.shape[2:]
    blocks = seq_vals.reshape((seq_vals.shape[0], 2 * CP_SIZE, CHUNK_LEN) + trailing)
    first_half = blocks[:, :CP_SIZE]
    second_half = jnp.flip(blocks[:, CP_SIZE:], axis=1)
    return jnp.stack([first_half, second_half], axis=2).reshape(seq_vals.shape)


def setup_inputs(seed: int = 0, part: int = 0) -> dict:
    part_key = jax.random.fold_in(jax.random.key(seed), part)
    draw_keys = jax.random.split(part_key, 5)
    weight_keys = jax.random.split(jax.random.key(seed + 1), 4)
    common = jax.random.normal(draw_keys[0], (BATCH_ROWS, 1, MODEL_DIM), jnp.float32)
    walk_steps = jax.random.normal(draw_keys[1], (BATCH_ROWS, SEQ_LEN, WALK_RANK), jnp.float32)
    walk_path = jnp.cumsum(walk_steps, axis=1) / math.sqrt(SEQ_LEN)
    walk_basis = jax.random.normal(draw_keys[2], (WALK_RANK, MODEL_DIM), jnp.float32) / math.sqrt(WALK_RANK)
    noise_part = jax.random.normal(draw_keys[3], (BATCH_ROWS, SEQ_LEN, MODEL_DIM), jnp.float32)
    x_seq = 0.5 * common + 0.8 * jnp.einsum('bsr,rd->bsd', walk_path, walk_basis) + 0.5 * noise_part
    pos_gaps = jax.random.randint(draw_keys[4], (BATCH_ROWS, SEQ_LEN), 1, 5, dtype=jnp.int32)
    pos_seq = jnp.cumsum(pos_gaps, axis=1, dtype=jnp.int32) - 1
    q_scale = 2.0 / math.sqrt(MODEL_DIM)
    in_scale = 1.0 / math.sqrt(MODEL_DIM)
    out_scale = 1.0 / math.sqrt(Q_HEADS * HEAD_DIM)
    w_query = jax.random.normal(weight_keys[0], (MODEL_DIM, Q_HEADS * HEAD_DIM), jnp.float32) * q_scale
    w_key = jax.random.normal(weight_keys[1], (MODEL_DIM, KV_HEADS * HEAD_DIM), jnp.float32) * in_scale
    w_value = jax.random.normal(weight_keys[2], (MODEL_DIM, KV_HEADS * HEAD_DIM), jnp.float32) * in_scale
    w_out = jax.random.normal(weight_keys[3], (Q_HEADS * HEAD_DIM, MODEL_DIM), jnp.float32) * out_scale
    return {
        'x': to_storage_order(x_seq).astype(jnp.bfloat16),
        'positions': to_storage_order(pos_seq),
        'w_query': w_query.astype(jnp.bfloat16),
        'w_key': w_key.astype(jnp.bfloat16),
        'w_value': w_value.astype(jnp.bfloat16),
        'w_out': w_out.astype(jnp.bfloat16),
    }


def rope_tables(pos_vals):
    inv_freq = jnp.asarray([ROPE_BASE ** (-2.0 * freq_idx / HEAD_DIM) for freq_idx in range(HEAD_DIM // 2)], dtype=jnp.float32)
    angles = pos_vals.astype(jnp.float32)[..., None] * inv_freq
    return jnp.cos(angles), jnp.sin(angles)


def apply_rope(head_vals, cos_t, sin_t):
    half_dim = head_vals.shape[-1] // 2
    lower_half = head_vals[..., :half_dim]
    upper_half = head_vals[..., half_dim:]
    return jnp.concatenate([lower_half * cos_t - upper_half * sin_t, upper_half * cos_t + lower_half * sin_t], axis=-1)


def attend_sequence(row_args):
    q_row, k_row, v_row, pos_row = row_args
    k_blocks = k_row.astype(jnp.float32).reshape(N_BLOCKS, CHUNK_LEN, KV_HEADS, HEAD_DIM)
    v_blocks = v_row.astype(jnp.float32).reshape(N_BLOCKS, CHUNK_LEN, KV_HEADS, HEAD_DIM)
    kpos_blocks = pos_row.reshape(N_BLOCKS, CHUNK_LEN)
    score_scale = 1.0 / math.sqrt(HEAD_DIM)

    def query_block(query_args):
        q_blk, qpos_blk = query_args
        q_f32 = q_blk.astype(jnp.float32)

        def block_scores(k_blk, kpos_blk):
            raw_scores = jnp.einsum('qhgd,khd->hgqk', q_f32, k_blk) * score_scale
            visible = kpos_blk[None, :] <= qpos_blk[:, None]
            return jnp.where(visible, raw_scores, -jnp.inf)

        def max_step(run_max, key_args):
            k_blk, kpos_blk = key_args
            return jnp.maximum(run_max, block_scores(k_blk, kpos_blk).max(axis=-1)), None

        init_max = jnp.full((KV_HEADS, Q_PER_KV, CHUNK_LEN), -jnp.inf, jnp.float32)
        row_max, _ = lax.scan(max_step, init_max, (k_blocks, kpos_blocks))

        def sum_step(loop_carry, key_args):
            run_sum, out_accum = loop_carry
            k_blk, v_blk, kpos_blk = key_args
            exp_scores = jnp.exp(block_scores(k_blk, kpos_blk) - row_max[..., None])
            rounded = exp_scores.astype(jnp.bfloat16).astype(jnp.float32)
            out_accum = out_accum + jnp.einsum('hgqk,khd->hgqd', rounded, v_blk)
            return (run_sum + exp_scores.sum(axis=-1), out_accum), None

        init_sum = jnp.zeros((KV_HEADS, Q_PER_KV, CHUNK_LEN), jnp.float32)
        init_accum = jnp.zeros((KV_HEADS, Q_PER_KV, CHUNK_LEN, HEAD_DIM), jnp.float32)
        (row_sum, out_accum), _ = lax.scan(sum_step, (init_sum, init_accum), (k_blocks, v_blocks, kpos_blocks))
        normed = (out_accum / row_sum[..., None]).astype(jnp.bfloat16)
        return jnp.transpose(normed, (2, 0, 1, 3)).reshape(CHUNK_LEN, Q_HEADS * HEAD_DIM)

    q_blocks = q_row.reshape(N_BLOCKS, CHUNK_LEN, KV_HEADS, Q_PER_KV, HEAD_DIM)
    out_blocks = lax.map(query_block, (q_blocks, pos_row.reshape(N_BLOCKS, CHUNK_LEN)))
    return out_blocks.reshape(SEQ_LEN, Q_HEADS * HEAD_DIM)


def reference(x, positions, w_query, w_key, w_value, w_out):
    flat_x = x.reshape(BATCH_ROWS * SEQ_LEN, MODEL_DIM)
    q_proj = jnp.dot(flat_x, w_query, preferred_element_type=jnp.float32).astype(jnp.bfloat16)
    k_proj = jnp.dot(flat_x, w_key, preferred_element_type=jnp.float32).astype(jnp.bfloat16)
    v_proj = jnp.dot(flat_x, w_value, preferred_element_type=jnp.float32).astype(jnp.bfloat16)
    cos_t, sin_t = rope_tables(positions)
    q_heads = q_proj.reshape(BATCH_ROWS, SEQ_LEN, KV_HEADS, Q_PER_KV, HEAD_DIM).astype(jnp.float32)
    q_rot = apply_rope(q_heads, cos_t[:, :, None, None, :], sin_t[:, :, None, None, :]).astype(jnp.bfloat16)
    k_heads = k_proj.reshape(BATCH_ROWS, SEQ_LEN, KV_HEADS, HEAD_DIM).astype(jnp.float32)
    k_rot = apply_rope(k_heads, cos_t[:, :, None, :], sin_t[:, :, None, :]).astype(jnp.bfloat16)
    v_heads = v_proj.reshape(BATCH_ROWS, SEQ_LEN, KV_HEADS, HEAD_DIM)
    attn_out = lax.map(attend_sequence, (q_rot, k_rot, v_heads, positions))
    out_proj = jnp.dot(attn_out.reshape(BATCH_ROWS * SEQ_LEN, Q_HEADS * HEAD_DIM), w_out, preferred_element_type=jnp.float32)
    return (x.astype(jnp.float32) + out_proj.reshape(BATCH_ROWS, SEQ_LEN, MODEL_DIM)).astype(jnp.bfloat16)
```

```python
import functools
import math
import jax
import jax.numpy as jnp
from jax import lax
from jax.experimental import pallas as pl
from jax.experimental.pallas import tpu as pltpu
from jax.sharding import PartitionSpec as P

HEAD_DIM = 128
ROPE_BASE = 500000
AXES = ('tp', 'cp')


def rope_tables(pos_vals):
    inv_freq = jnp.asarray([ROPE_BASE ** (-2.0 * freq_idx / HEAD_DIM) for freq_idx in range(HEAD_DIM // 2)], dtype=jnp.float32)
    angles = pos_vals.astype(jnp.float32)[..., None] * inv_freq
    cos_t, sin_t = jnp.cos(angles), jnp.sin(angles)
    return jnp.concatenate([cos_t, cos_t], axis=-1), jnp.concatenate([-sin_t, sin_t], axis=-1)


def rotate(head_vals, cos_t, sin_t):
    wide = head_vals.astype(jnp.float32)
    return (wide * cos_t + pltpu.roll(wide, HEAD_DIM // 2, 1) * sin_t).astype(jnp.bfloat16)


def rope_own_body(k_ref, v_ref, cos_ref, sin_ref, kv_ref):
    width = k_ref.shape[1]
    for col in range(0, width, HEAD_DIM):
        kv_ref[:, col:col + HEAD_DIM] = rotate(k_ref[:, col:col + HEAD_DIM], cos_ref[...], sin_ref[...])
    kv_ref[:, width:] = v_ref[...]


def rope_other_body(core_ref, near_ref, far_ref, cos_ref, sin_ref, kv_ref):
    width = near_ref.shape[1]
    half = width // 2
    for src_ref, slot in ((near_ref, core_ref[0]), (far_ref, 1 - core_ref[0])):
        for col in range(0, half, HEAD_DIM):
            at = pl.multiple_of(slot * half + col, HEAD_DIM)
            kv_ref[:, pl.ds(at, HEAD_DIM)] = rotate(src_ref[:, col:col + HEAD_DIM], cos_ref[...], sin_ref[...])
        at = pl.multiple_of(width + slot * half, HEAD_DIM)
        kv_ref[:, pl.ds(at, half)] = src_ref[:, half:]


def rope_own(k_proj, v_proj, cos_t, sin_t, block):
    rows, width = k_proj.shape
    spec = lambda cols: pl.BlockSpec((block, cols), lambda i: (i, 0))
    return pl.pallas_call(
        rope_own_body, grid=(rows // block,),
        in_specs=[spec(width), spec(width), spec(HEAD_DIM), spec(HEAD_DIM)], out_specs=spec(2 * width),
        out_shape=jax.ShapeDtypeStruct((rows, 2 * width), jnp.bfloat16),
        cost_estimate=pl.CostEstimate(flops=rows * width * 40, bytes_accessed=rows * width * 10, transcendentals=0),
        name='rope_own')(k_proj, v_proj, cos_t, sin_t)


def rope_other(core, near, far, cos_t, sin_t, block):
    rows, width = near.shape
    spec = lambda cols: pl.BlockSpec((block, cols), lambda i, *_: (i, 0))
    return pl.pallas_call(
        rope_other_body,
        grid_spec=pltpu.PrefetchScalarGridSpec(
            num_scalar_prefetch=1, grid=(rows // block,),
            in_specs=[spec(width), spec(width), spec(HEAD_DIM), spec(HEAD_DIM)], out_specs=spec(2 * width)),
        out_shape=jax.ShapeDtypeStruct((rows, 2 * width), jnp.bfloat16),
        cost_estimate=pl.CostEstimate(flops=rows * width * 40, bytes_accessed=rows * width * 10, transcendentals=0),
        name='rope_other')(core, near, far, cos_t, sin_t)


def attend_body(n_q, groups_each, q_per_kv, n_kv, flag_ref, *refs):
    q_refs = refs[:n_q]
    cos_ref, sin_ref = refs[n_q:n_q + 2]
    slots = refs[n_q + 2:n_q + 10]
    out_ref = refs[n_q + 10]
    s_refs = refs[n_q + 11:n_q + 13]
    p_refs = refs[n_q + 13:n_q + 15]
    block = cos_ref.shape[0]
    scale = 1.0 / math.sqrt(HEAD_DIM)
    kv_cols = n_kv * HEAD_DIM

    def run(use):
        keys = len(use) * block
        work = [(q_ref, idx) for q_ref in q_refs for idx in range(groups_each)]
        off = jnp.float32(-jnp.inf)
        bias_b = jnp.where(flag_ref[1] == 1, jnp.float32(0), off)
        bias_cd = jnp.where(flag_ref[2] == 1, jnp.float32(0), off)
        row_id = lax.broadcasted_iota(jnp.int32, (block, block), 0)
        col_id = lax.broadcasted_iota(jnp.int32, (block, block), 1)
        seen = col_id <= row_id

        def score(step):
            q_ref, idx = work[step]
            base = idx * q_per_kv * HEAD_DIM
            heads = [rotate(q_ref[:, base + h * HEAD_DIM:base + (h + 1) * HEAD_DIM], cos_ref[...], sin_ref[...]) for h in range(q_per_kv)]
            q_all = jnp.concatenate(heads, axis=0)
            at = pl.multiple_of(flag_ref[3 + step] * HEAD_DIM, HEAD_DIM)
            k_all = jnp.concatenate([slots[u][:, pl.ds(at, HEAD_DIM)] for u in use], axis=0)
            s_refs[step % 2][:, :keys] = lax.dot_general(q_all, k_all, (((1,), (1,)), ((), ())), preferred_element_type=jnp.float32)

        def soft(step):
            s_ref, p_ref = s_refs[step % 2], p_refs[step % 2]
            sums = []
            for h in range(q_per_kv):
                rows = slice(h * block, (h + 1) * block)
                tiles = []
                for n, u in enumerate(use):
                    tile = s_ref[rows, n * block:(n + 1) * block]
                    if u == 0:
                        tile = jnp.where(seen, tile, off)
                    elif u == 1:
                        tile = tile + bias_b
                    elif u in (2, 3):
                        tile = tile + bias_cd
                    tiles.append(tile)
                top = functools.reduce(jnp.maximum, tiles).max(axis=1, keepdims=True)
                total = None
                for n, tile in enumerate(tiles):
                    e = jnp.exp((tile - top) * scale)
                    total = e if total is None else total + e
                    p_ref[rows, n * block:(n + 1) * block] = e.astype(jnp.bfloat16)
                sums.append(total.sum(axis=1, keepdims=True))
            return sums

        def finish(step, sums):
            p_ref = p_refs[step % 2]
            at = pl.multiple_of(kv_cols + flag_ref[3 + step] * HEAD_DIM, HEAD_DIM)
            v_all = jnp.concatenate([slots[u][:, pl.ds(at, HEAD_DIM)] for u in use], axis=0)
            o_all = jnp.dot(p_ref[:, :keys], v_all, preferred_element_type=jnp.float32)
            for h in range(q_per_kv):
                col = (step * q_per_kv + h) * HEAD_DIM
                out_ref[:, col:col + HEAD_DIM] = (o_all[h * block:(h + 1) * block] / sums[h]).astype(jnp.bfloat16)

        score(0)
        for step in range(len(work)):
            if step + 1 < len(work):
                score(step + 1)
            sums = soft(step)
            finish(step, sums)

    @pl.when(flag_ref[0] == 1)
    def _():
        run((0, 1, 2, 3, 4, 5, 6, 7))

    @pl.when(flag_ref[0] == 0)
    def _():
        run((0, 1, 2, 3))


def attend(flags, q_list, cos_t, sin_t, slots, block, q_per_kv):
    rows = cos_t.shape[0]
    n_q = len(q_list)
    width = q_list[0].shape[1]
    groups_each = width // (q_per_kv * HEAD_DIM)
    n_kv = slots[0].shape[1] // (2 * HEAD_DIM)
    kv_width = slots[0].shape[1]
    here = lambda cols: pl.BlockSpec((block, cols), lambda i, f: (i, 0))
    gated = lambda idx: pl.BlockSpec((block, kv_width), lambda i, f: (i * f[idx], 0))
    slot_specs = [here(kv_width), gated(1), gated(2), gated(2), gated(0), gated(0), gated(0), gated(0)]
    stack = q_per_kv * block
    flops = 4 * rows * width * n_q * 8 * block
    return pl.pallas_call(
        functools.partial(attend_body, n_q, groups_each, q_per_kv, n_kv),
        grid_spec=pltpu.PrefetchScalarGridSpec(
            num_scalar_prefetch=1, grid=(rows // block,),
            in_specs=[here(width)] * n_q + [here(HEAD_DIM), here(HEAD_DIM)] + slot_specs,
            out_specs=here(width * n_q),
            scratch_shapes=[pltpu.VMEM((stack, 8 * block), jnp.float32)] * 2 + [pltpu.VMEM((stack, 8 * block), jnp.bfloat16)] * 2),
        out_shape=jax.ShapeDtypeStruct((rows, width * n_q), jnp.bfloat16),
        compiler_params=pltpu.CompilerParams(vmem_limit_bytes=56 * 1024 * 1024),
        cost_estimate=pl.CostEstimate(flops=flops * 2, bytes_accessed=rows * (width * n_q * 4 + 8 * kv_width * 2), transcendentals=rows * width * n_q * 8))(flags, *q_list, cos_t, sin_t, *slots)


def gather_dot_body(n_w, has_x, o_ref, *refs):
    w_refs = refs[:n_w]
    acc_ref = refs[n_w]
    out_ref = refs[-1]
    depth = w_refs[0].shape[0]
    rows = o_ref.shape[0]
    step = min(512, rows)
    for top in range(0, rows, step):
        part = slice(top, top + step)
        total = acc_ref[part, :]
        for j in range(n_w):
            total = total + jnp.dot(o_ref[part, j * depth:(j + 1) * depth], w_refs[j][...], preferred_element_type=jnp.float32)
        if has_x:
            total = refs[n_w + 1][part, :].astype(jnp.float32) + total
        out_ref[part, :] = total.astype(out_ref.dtype)


def gather_dot(o_vals, w_list, acc, x_rows):
    rows, depth_all = o_vals.shape
    depth, cols = w_list[0].shape
    tile = 512
    tall = pl.BlockSpec((rows, tile), lambda i: (0, i))
    args = [o_vals, *w_list, acc] + ([x_rows] if x_rows is not None else [])
    specs = [pl.BlockSpec((rows, depth_all), lambda i: (0, 0))] + [pl.BlockSpec((depth, tile), lambda i: (0, i))] * len(w_list) + [tall] * (len(args) - 1 - len(w_list))
    return pl.pallas_call(
        functools.partial(gather_dot_body, len(w_list), x_rows is not None),
        grid=(cols // tile,), in_specs=specs, out_specs=tall,
        out_shape=jax.ShapeDtypeStruct((rows, cols), jnp.float32 if x_rows is None else jnp.bfloat16),
        compiler_params=pltpu.CompilerParams(vmem_limit_bytes=58 * 1024 * 1024),
        cost_estimate=pl.CostEstimate(flops=2 * rows * depth_all * cols, bytes_accessed=rows * cols * 8, transcendentals=0))(*args)


def solution(mesh):
    cp_size = mesh.shape['cp']
    row_spec = P('data', ('cp', 'tp'))
    flat = lambda c, t: t * cp_size + c
    swap_y = [(flat(c, t), flat(c, 1 - t)) for c in range(cp_size) for t in range(2)]
    swap_x = [(flat(c, t), flat(c ^ 2, t)) for c in range(cp_size) for t in range(2)]
    swap_d = [(flat(c, t), flat(c ^ 1, t)) for c in range(cp_size) for t in range(2)]
    own_d = [(flat(0, 0), flat(1, 0)), (flat(2, 0), flat(3, 0)), (flat(1, 1), flat(0, 1)), (flat(3, 1), flat(2, 1))]
    own_x = [(flat(0, 0), flat(2, 0)), (flat(1, 0), flat(3, 0)), (flat(2, 1), flat(0, 1)), (flat(3, 1), flat(1, 1))]
    own_xd = [(flat(2, 0), flat(3, 0)), (flat(3, 0), flat(2, 0)), (flat(0, 1), flat(1, 1)), (flat(1, 1), flat(0, 1))]
    up_y = [(flat(c, 0), flat(c, 1)) for c in range(cp_size)]
    up_x = [(flat(c, 1), flat(c ^ 2, 1)) for c in range(cp_size)]
    up_d = [(flat(c, 1), flat(c ^ 1, 1)) for c in range(cp_size)]

    def move(vals, pairs):
        return lax.ppermute(vals, AXES, pairs)

    def after(vals, *others):
        return lax.optimization_barrier((vals, *others))[0]

    def block_fn(x_rows, pos_rows, w_query, w_key, w_value, w_out):
        batch, block, dim = x_rows.shape
        rows = batch * block
        kv_local = w_key.shape[1] // HEAD_DIM
        q_per_kv = w_query.shape[1] // w_key.shape[1]
        group = q_per_kv * HEAD_DIM
        c_idx, t_idx = lax.axis_index('cp'), lax.axis_index('tp')
        core = c_idx % 2
        x2 = x_rows.reshape(rows, dim)
        cos_t, sin_t = (tab.reshape(rows, HEAD_DIM) for tab in rope_tables(pos_rows))

        def project(weights):
            return jnp.dot(x2, weights, preferred_element_type=jnp.float32).astype(jnp.bfloat16)

        half = w_key.shape[1] // 2
        kv_send = jnp.concatenate([lax.dynamic_slice_in_dim(w_key, core * half, half, 1),
                                   lax.dynamic_slice_in_dim(w_value, core * half, half, 1)], axis=1)
        kv_near = move(kv_send, swap_y)

        kv_own = rope_own(project(w_key), project(w_value), cos_t, sin_t, block)
        q_own = project(w_query)
        kv_near = after(kv_near, q_own)
        kv_far = move(kv_near, swap_d)
        kv_oth = rope_other(core.reshape(1).astype(jnp.int32), project(kv_near), project(kv_far), cos_t, sin_t, block)

        c_own = move(kv_own, own_x)
        b_own = move(kv_own, own_d)
        d_own = move(c_own, own_xd)
        e_oth = move(kv_own, up_y)
        c_oth = move(kv_oth, own_x)
        b_oth = move(kv_oth, own_d)
        d_oth = move(c_oth, own_xd)
        e_own = move(kv_oth, up_y)
        f_oth = move(e_oth, up_d)
        g_oth = move(e_oth, up_x)
        h_oth = move(g_oth, up_d)
        f_own = move(e_own, up_d)
        g_own = move(e_own, up_x)
        h_own = move(g_own, up_d)
        slots_own = (kv_own, b_own, c_own, d_own, e_own, f_own, g_own, h_own)
        slots_oth = (kv_oth, b_oth, c_oth, d_oth, e_oth, f_oth, g_oth, h_oth)

        wq_send = lax.dynamic_slice_in_dim(w_query, c_idx * group, group, 1)
        wq0 = move(wq_send, swap_y)
        wq2 = move(wq0, swap_d)
        wq1 = move(wq0, swap_x)
        wq3 = move(wq1, swap_d)
        wo_send = lax.dynamic_slice_in_dim(w_out, c_idx * group, group, 0)
        wo0 = move(wo_send, swap_y)
        wo2 = move(wo0, swap_d)
        wo1 = move(wo0, swap_x)
        wo3 = move(wo1, swap_d)

        use_b = jnp.where(t_idx == 0, core, 1 - core)
        use_cd = jnp.where(t_idx == 0, c_idx // 2, 1 - c_idx // 2)
        head_flags = [t_idx, use_b, use_cd]
        flags = lambda *groups: jnp.stack([jnp.asarray(f, jnp.int32) for f in head_flags + list(groups)])

        o_own = attend(flags(*range(kv_local)), [q_own], cos_t, sin_t, slots_own, block, q_per_kv)
        acc = jnp.dot(o_own, w_out, preferred_element_type=jnp.float32)
        wq0, wq2, acc = lax.optimization_barrier((wq0, wq2, acc))
        o_near = attend(flags(c_idx, c_idx ^ 1), [project(wq0), project(wq2)], cos_t, sin_t, slots_oth, block, q_per_kv)
        acc = gather_dot(o_near, [wo0, wo2], acc, None)
        wq1, wq3, acc = lax.optimization_barrier((wq1, wq3, acc))
        q_far = [project(wq1), project(wq3)]
        o_far = attend(flags(c_idx ^ 2, c_idx ^ 3), q_far, cos_t, sin_t, slots_oth, block, q_per_kv)
        y_rows = gather_dot(o_far, [wo1, wo3], acc, x2)
        return y_rows.reshape(x_rows.shape)

    return jax.shard_map(block_fn, mesh=mesh,
                         in_specs=(row_spec, row_spec, P(None, 'tp'), P(None, 'tp'), P(None, 'tp'), P('tp', None)),
                         out_specs=row_spec, check_vma=False)
```

```python
import functools
import math
import jax
import jax.numpy as jnp
from jax import lax
from jax.experimental import pallas as pl
from jax.experimental.pallas import tpu as pltpu
from jax.sharding import PartitionSpec as P

HEAD_DIM = 128
ROPE_BASE = 500000
AXES = ('tp', 'cp')


def rope_tables(pos_vals):
    inv_freq = jnp.asarray([ROPE_BASE ** (-2.0 * freq_idx / HEAD_DIM) for freq_idx in range(HEAD_DIM // 2)], dtype=jnp.float32)
    angles = pos_vals.astype(jnp.float32)[..., None] * inv_freq
    cos_t, sin_t = jnp.cos(angles), jnp.sin(angles)
    return jnp.concatenate([cos_t, cos_t], axis=-1), jnp.concatenate([-sin_t, sin_t], axis=-1)


def rotate(head_vals, cos_t, sin_t):
    wide = head_vals.astype(jnp.float32)
    return (wide * cos_t + pltpu.roll(wide, HEAD_DIM // 2, 1) * sin_t).astype(jnp.bfloat16)


def rope_own_body(k_ref, v_ref, cos_ref, sin_ref, kv_ref):
    width = k_ref.shape[1]
    for col in range(0, width, HEAD_DIM):
        kv_ref[:, col:col + HEAD_DIM] = rotate(k_ref[:, col:col + HEAD_DIM], cos_ref[...], sin_ref[...])
    kv_ref[:, width:] = v_ref[...]


def rope_other_body(core_ref, near_ref, far_ref, cos_ref, sin_ref, kv_ref):
    width = near_ref.shape[1]
    half = width // 2
    for src_ref, slot in ((near_ref, core_ref[0]), (far_ref, 1 - core_ref[0])):
        for col in range(0, half, HEAD_DIM):
            at = pl.multiple_of(slot * half + col, HEAD_DIM)
            kv_ref[:, pl.ds(at, HEAD_DIM)] = rotate(src_ref[:, col:col + HEAD_DIM], cos_ref[...], sin_ref[...])
        at = pl.multiple_of(width + slot * half, HEAD_DIM)
        kv_ref[:, pl.ds(at, half)] = src_ref[:, half:]


def rope_own(k_proj, v_proj, cos_t, sin_t, block):
    rows, width = k_proj.shape
    spec = lambda cols: pl.BlockSpec((block, cols), lambda i: (i, 0))
    return pl.pallas_call(
        rope_own_body, grid=(rows // block,),
        in_specs=[spec(width), spec(width), spec(HEAD_DIM), spec(HEAD_DIM)], out_specs=spec(2 * width),
        out_shape=jax.ShapeDtypeStruct((rows, 2 * width), jnp.bfloat16),
        cost_estimate=pl.CostEstimate(flops=rows * width * 40, bytes_accessed=rows * width * 10, transcendentals=0),
        name='rope_own')(k_proj, v_proj, cos_t, sin_t)


def rope_other(core, near, far, cos_t, sin_t, block):
    rows, width = near.shape
    spec = lambda cols: pl.BlockSpec((block, cols), lambda i, *_: (i, 0))
    return pl.pallas_call(
        rope_other_body,
        grid_spec=pltpu.PrefetchScalarGridSpec(
            num_scalar_prefetch=1, grid=(rows // block,),
            in_specs=[spec(width), spec(width), spec(HEAD_DIM), spec(HEAD_DIM)], out_specs=spec(2 * width)),
        out_shape=jax.ShapeDtypeStruct((rows, 2 * width), jnp.bfloat16),
        cost_estimate=pl.CostEstimate(flops=rows * width * 40, bytes_accessed=rows * width * 10, transcendentals=0),
        name='rope_other')(core, near, far, cos_t, sin_t)


CHUNK = 32
EXP_SCALE = math.log2(math.e) / math.sqrt(HEAD_DIM)


def slot_cols(slots, col):
    at = pl.multiple_of(col * HEAD_DIM, HEAD_DIM)
    return jnp.concatenate([slot[:, pl.ds(at, HEAD_DIM)] for slot in slots], axis=0)


def attend_body(mode, n_slots, n_q, groups_each, q_per_kv, n_kv, flag_ref, *refs):
    late = mode != 'first'
    q_refs, refs = refs[:n_q], refs[n_q:]
    (cos_ref, sin_ref), refs = refs[:2], refs[2:]
    if late:
        (old_part_ref, old_log_ref), refs = refs[:2], refs[2:]
    slots, refs = refs[:n_slots], refs[n_slots:]
    if mode == 'last':
        (out_ref,), refs = refs[:1], refs[1:]
    else:
        (part_ref, log_ref, turned_ref), refs = refs[:3], refs[3:]
    s_refs, p_refs, top_refs, sum_refs = refs[:2], refs[2:4], refs[4:6], refs[6:8]
    block = cos_ref.shape[0]
    work = [(q_ref, idx) for q_ref in q_refs for idx in range(groups_each)]
    off = jnp.float32(-jnp.inf)
    bias_b = jnp.where(flag_ref[1] == 1, jnp.float32(0), off)
    bias_cd = jnp.where(flag_ref[2] == 1, jnp.float32(0), off)
    col_id = lax.broadcasted_iota(jnp.int32, (CHUNK, block), 1)
    row_id = lax.broadcasted_iota(jnp.int32, (CHUNK, block), 0)

    def score(step):
        q_ref, idx = work[step]
        heads = []
        for h in range(q_per_kv):
            at = (idx * q_per_kv + h) * HEAD_DIM
            head = q_ref[:, at:at + HEAD_DIM]
            if not late:
                head = rotate(head, cos_ref[...], sin_ref[...])
                to = (step * q_per_kv + h) * HEAD_DIM
                turned_ref[:, to:to + HEAD_DIM] = head
            heads.append(head)
        q_all = jnp.concatenate(heads, axis=0)
        k_all = slot_cols(slots, flag_ref[3 + step])
        s_refs[step % 2][...] = lax.dot_general(q_all, k_all, (((1,), (1,)), ((), ())), preferred_element_type=jnp.float32)

    def soft(step):
        s_ref, p_ref, top_ref, sum_ref = s_refs[step % 2], p_refs[step % 2], top_refs[step % 2], sum_refs[step % 2]
        for h in range(q_per_kv):
            for low in range(0, block, CHUNK):
                rows = slice(h * block + low, h * block + low + CHUNK)
                tiles = [s_ref[rows, n * block:(n + 1) * block] for n in range(n_slots)]
                if late:
                    top = functools.reduce(jnp.maximum, tiles)
                else:
                    tiles[0] = jnp.where(col_id <= row_id + low, tiles[0], off)
                    top = jnp.maximum(jnp.maximum(tiles[0], tiles[1] + bias_b), jnp.maximum(tiles[2], tiles[3]) + bias_cd)
                top = jnp.broadcast_to(top.max(axis=1, keepdims=True), top.shape) * EXP_SCALE
                shifts = [top] * n_slots if late else [top, top - bias_b, top - bias_cd, top - bias_cd]
                total = None
                for n, tile in enumerate(tiles):
                    e = jnp.exp2(tile * EXP_SCALE - shifts[n])
                    total = e if total is None else total + e
                    p_ref[rows, n * block:(n + 1) * block] = e.astype(jnp.bfloat16)
                top_ref[rows, :] = top
                sum_ref[rows, :] = jnp.broadcast_to(total.sum(axis=1, keepdims=True), top.shape)

    def finish(step):
        top_ref, sum_ref = top_refs[step % 2], sum_refs[step % 2]
        v_all = slot_cols(slots, n_kv + flag_ref[3 + step])
        o_all = jnp.dot(p_refs[step % 2][...], v_all, preferred_element_type=jnp.float32)
        for h in range(q_per_kv):
            rows = slice(h * block, (h + 1) * block)
            cols = slice((step * q_per_kv + h) * HEAD_DIM, (step * q_per_kv + h + 1) * HEAD_DIM)
            if late:
                old, new = old_log_ref[:, cols], top_ref[rows, :]
                peak = jnp.maximum(old, new)
                old, new = jnp.exp2(old - peak), jnp.exp2(new - peak)
                mixed = old_part_ref[:, cols] * old + o_all[rows] * new
                total = old + sum_ref[rows, :] * new
                out_ref[:, cols] = (mixed / total).astype(jnp.bfloat16)
            else:
                total = sum_ref[rows, :]
                part_ref[:, cols] = o_all[rows] / total
                log_ref[:, cols] = top_ref[rows, :] + jnp.log(total) * math.log2(math.e)

    def run():
        score(0)
        for step in range(len(work)):
            if step + 1 < len(work):
                score(step + 1)
            soft(step)
            finish(step)

    if not late:
        run()
    else:
        pl.when(flag_ref[0] == 1)(run)

        @pl.when(flag_ref[0] == 0)
        def _():
            out_ref[...] = old_part_ref[...].astype(jnp.bfloat16)


def attend(flags, q_list, cos_t, sin_t, slots, block, q_per_kv, state, mode):
    rows = cos_t.shape[0]
    n_q = len(q_list)
    width = q_list[0].shape[1]
    groups_each = width // (q_per_kv * HEAD_DIM)
    kv_width = slots[0].shape[1]
    n_kv = kv_width // (2 * HEAD_DIM)
    here = lambda cols: pl.BlockSpec((block, cols), lambda i, f: (i, 0))
    gated = lambda idx: pl.BlockSpec((block, kv_width), lambda i, f: (i * f[idx], 0))
    all_q = width * n_q
    wide = jax.ShapeDtypeStruct((rows, all_q), jnp.float32)
    extra = [] if state is None else list(state)
    slot_specs = [here(kv_width), gated(1), gated(2), gated(2)] if state is None else [gated(0)] * len(slots)
    out_shape = jax.ShapeDtypeStruct((rows, all_q), jnp.bfloat16) if mode == 'last' else [wide, wide, jax.ShapeDtypeStruct((rows, all_q), jnp.bfloat16)]
    out_specs = here(all_q) if mode == 'last' else [here(all_q)] * 3
    keys = len(slots) * block
    stack = q_per_kv * block
    return pl.pallas_call(
        functools.partial(attend_body, mode, len(slots), n_q, groups_each, q_per_kv, n_kv),
        grid_spec=pltpu.PrefetchScalarGridSpec(
            num_scalar_prefetch=1, grid=(rows // block,),
            in_specs=[here(width)] * n_q + [here(HEAD_DIM), here(HEAD_DIM)] + [here(all_q)] * len(extra) + slot_specs,
            out_specs=out_specs,
            scratch_shapes=[pltpu.VMEM((stack, keys), jnp.float32)] * 2 + [pltpu.VMEM((stack, keys), jnp.bfloat16)] * 2
            + [pltpu.VMEM((stack, HEAD_DIM), jnp.float32)] * 4),
        out_shape=out_shape,
        compiler_params=pltpu.CompilerParams(vmem_limit_bytes=60 * 1024 * 1024),
        cost_estimate=pl.CostEstimate(flops=16 * rows * all_q * keys, bytes_accessed=rows * (all_q * 6 + 4 * kv_width * 2), transcendentals=rows * all_q * 4))(flags, *q_list, cos_t, sin_t, *extra, *slots)


def gather_dot_body(plan, n_o, n_w, n_first, *refs):
    o_refs, w_refs = refs[:n_o], refs[n_o:n_o + n_w]
    first_ref, second_ref, x_ref, out_ref = refs[n_o + n_w:]
    rows = x_ref.shape[0]
    step = min(512, rows)
    in_first = pl.program_id(0) < n_first
    for top in range(0, rows, step):
        part = slice(top, top + step)
        total = jnp.where(in_first, first_ref[part, :], second_ref[part, :])
        for pieces, w_at in plan:
            lhs = [o_refs[o_at][part, col:col + width] for o_at, col, width in pieces]
            lhs = jnp.concatenate(lhs, axis=1) if len(lhs) > 1 else lhs[0]
            total = total + jnp.dot(lhs, w_refs[w_at][...], preferred_element_type=jnp.float32)
        out_ref[part, :] = (x_ref[part, :].astype(jnp.float32) + total).astype(out_ref.dtype)


def gather_dot(plan, o_list, w_list, accs, x_rows):
    rows, cols = x_rows.shape
    tile = 512
    tall = pl.BlockSpec((rows, tile), lambda i: (0, i))
    n_first = accs[0].shape[1] // tile
    acc_specs = [pl.BlockSpec((rows, tile), lambda i: (0, jnp.minimum(i, n_first - 1))), pl.BlockSpec((rows, tile), lambda i: (0, jnp.maximum(i - n_first, 0)))]
    depth_all = sum(w.shape[0] for w in w_list)
    specs = [pl.BlockSpec(o.shape, lambda i: (0, 0)) for o in o_list] + [pl.BlockSpec((w.shape[0], tile), lambda i: (0, i)) for w in w_list] + acc_specs + [tall]
    return pl.pallas_call(
        functools.partial(gather_dot_body, plan, len(o_list), len(w_list), n_first),
        grid=(cols // tile,), in_specs=specs, out_specs=tall,
        out_shape=jax.ShapeDtypeStruct((rows, cols), jnp.bfloat16),
        compiler_params=pltpu.CompilerParams(vmem_limit_bytes=62 * 1024 * 1024),
        cost_estimate=pl.CostEstimate(flops=2 * rows * depth_all * cols, bytes_accessed=rows * cols * 8, transcendentals=0))(*o_list, *w_list, *accs, x_rows)


def solution(mesh):
    cp_size = mesh.shape['cp']
    row_spec = P('data', ('cp', 'tp'))
    flat = lambda c, t: t * cp_size + c
    swap_y = [(flat(c, t), flat(c, 1 - t)) for c in range(cp_size) for t in range(2)]
    swap_x = [(flat(c, t), flat(c ^ 2, t)) for c in range(cp_size) for t in range(2)]
    swap_d = [(flat(c, t), flat(c ^ 1, t)) for c in range(cp_size) for t in range(2)]
    own_d = [(flat(0, 0), flat(1, 0)), (flat(2, 0), flat(3, 0)), (flat(1, 1), flat(0, 1)), (flat(3, 1), flat(2, 1))]
    own_x = [(flat(0, 0), flat(2, 0)), (flat(1, 0), flat(3, 0)), (flat(2, 1), flat(0, 1)), (flat(3, 1), flat(1, 1))]
    own_xd = [(flat(2, 0), flat(3, 0)), (flat(3, 0), flat(2, 0)), (flat(0, 1), flat(1, 1)), (flat(1, 1), flat(0, 1))]
    up_y = [(flat(c, 0), flat(c, 1)) for c in range(cp_size)]
    up_x = [(flat(c, 1), flat(c ^ 2, 1)) for c in range(cp_size)]
    up_d = [(flat(c, 1), flat(c ^ 1, 1)) for c in range(cp_size)]

    def move(vals, pairs):
        return lax.ppermute(vals, AXES, pairs)

    def after(vals, *others):
        return lax.optimization_barrier((vals, *others))[0]

    def block_fn(x_rows, pos_rows, w_query, w_key, w_value, w_out):
        batch, block, dim = x_rows.shape
        rows = batch * block
        kv_local = w_key.shape[1] // HEAD_DIM
        q_per_kv = w_query.shape[1] // w_key.shape[1]
        group = q_per_kv * HEAD_DIM
        c_idx, t_idx = lax.axis_index('cp'), lax.axis_index('tp')
        core = c_idx % 2
        x2 = x_rows.reshape(rows, dim)
        cos_t, sin_t = (tab.reshape(rows, HEAD_DIM) for tab in rope_tables(pos_rows))

        def project(weights):
            return jnp.dot(x2, weights, preferred_element_type=jnp.float32).astype(jnp.bfloat16)

        half = w_key.shape[1] // 2
        kv_send = jnp.concatenate([lax.dynamic_slice_in_dim(w_key, core * half, half, 1),
                                   lax.dynamic_slice_in_dim(w_value, core * half, half, 1)], axis=1)
        kv_near = move(kv_send, swap_y)

        kv_own = rope_own(project(w_key), project(w_value), cos_t, sin_t, 4 * block)
        split = w_query.shape[1] // 2
        q_own_a = project(w_query[:, :split])
        kv_near = after(kv_near, q_own_a)
        kv_far = move(kv_near, swap_d)
        kv_oth = rope_other(core.reshape(1).astype(jnp.int32), project(kv_near), project(kv_far), cos_t, sin_t, 4 * block)

        q_own = [q_own_a, project(w_query[:, split:])]
        c_own = move(kv_own, own_x)
        b_own = move(kv_own, own_d)
        d_own = move(c_own, own_xd)
        e_oth = move(kv_own, up_y)
        c_oth = move(kv_oth, own_x)
        b_oth = move(kv_oth, own_d)
        d_oth = move(c_oth, own_xd)
        e_own = move(kv_oth, up_y)
        f_oth = move(e_oth, up_d)
        g_oth = move(e_oth, up_x)
        h_oth = move(g_oth, up_d)
        f_own = move(e_own, up_d)
        g_own = move(e_own, up_x)
        h_own = move(g_own, up_d)
        slots_own = (kv_own, b_own, c_own, d_own, e_own, f_own, g_own, h_own)
        slots_oth = (kv_oth, b_oth, c_oth, d_oth, e_oth, f_oth, g_oth, h_oth)

        wq_send = lax.dynamic_slice_in_dim(w_query, c_idx * group, group, 1)
        wq0 = move(wq_send, swap_y)
        wq2 = move(wq0, swap_d)
        wq1 = move(wq0, swap_x)
        wq3 = move(wq1, swap_d)
        use_b = jnp.where(t_idx == 0, core, 1 - core)
        use_cd = jnp.where(t_idx == 0, c_idx // 2, 1 - c_idx // 2)
        head_flags = [t_idx, use_b, use_cd]
        flags = lambda *groups: jnp.stack([jnp.asarray(f, jnp.int32) for f in head_flags + list(groups)])

        own_flags, near_flags, far_flags = flags(*range(kv_local)), flags(c_idx, c_idx ^ 1), flags(c_idx ^ 2, c_idx ^ 3)
        *state_own, turned_own = attend(own_flags, q_own, cos_t, sin_t, slots_own[:4], block, q_per_kv, None, 'first')
        q_near = [project(wq) for wq in (wq0, wq2)]
        *state_near, turned_near = attend(near_flags, q_near, cos_t, sin_t, slots_oth[:4], block, q_per_kv, None, 'first')
        w_out_late = after(w_out, state_near[1])
        pair, single = 2 * HEAD_DIM, HEAD_DIM
        part = group - pair - single

        def w_rows(groups, low, size):
            return jnp.concatenate([lax.dynamic_slice_in_dim(w_out_late, at * group + low, size, 0) for at in groups], axis=0)

        wo0 = move(w_rows([c_idx], pair + single, part), swap_y)
        wo2 = move(wo0, swap_d)
        wo1 = move(wo0, swap_x)
        wo3 = move(wo1, swap_d)
        wa0 = move(w_rows([c_idx, c_idx ^ 2], 0, pair), swap_y)
        wa2 = move(wa0, swap_d)
        wb0 = move(w_rows([c_idx, c_idx ^ 2], pair, single), swap_y)
        wb2 = move(wb0, swap_d)
        q_far = [project(wq) for wq in (wq1, wq3)]
        *state_far, turned_far = attend(far_flags, q_far, cos_t, sin_t, slots_oth[:4], block, q_per_kv, None, 'first')
        o_own = attend(own_flags, [turned_own], cos_t, sin_t, slots_own[4:], block, q_per_kv, state_own, 'last')
        dot32 = lambda o, w: jnp.dot(o, w, preferred_element_type=jnp.float32)
        cut = w_out.shape[1] // 5 * 3
        acc_a = dot32(o_own, w_out[:, :cut])
        acc_b = dot32(o_own, w_out[:, cut:])
        o_near = attend(near_flags, [turned_near], cos_t, sin_t, slots_oth[4:], block, q_per_kv, state_near, 'last')
        o_far = attend(far_flags, [turned_far], cos_t, sin_t, slots_oth[4:], block, q_per_kv, state_far, 'last')
        plan = []
        for place in (0, group):
            plan.append((((0, place, pair), (1, place, pair)), len(plan)))
            plan.append((((0, place + pair, single), (1, place + pair, single)), len(plan)))
            for o_at in (0, 1):
                plan.append((((o_at, place + pair + single, part),), len(plan)))
        y_rows = gather_dot(tuple(plan), [o_near, o_far], [wa0, wb0, wo0, wo1, wa2, wb2, wo2, wo3], (acc_a, acc_b), x2)
        return y_rows.reshape(x_rows.shape)

    return jax.shard_map(block_fn, mesh=mesh,
                         in_specs=(row_spec, row_spec, P(None, 'tp'), P(None, 'tp'), P(None, 'tp'), P('tp', None)),
                         out_specs=row_spec, check_vma=False)
```
